256 devices in a mesh: tm: 128 (over y, z, x), batch: 2 (over core).
Axes of the slice: x: 4, y: 4, z: 8, core: 2. Of those that a mesh axis runs over, the one named last changes fastest.
Arguments:
- gate_in: bfloat16 [8192, 4096], P('tm', 'batch'), parts along dimension 1, may hold values from -4.5 to 8.75
- cand_in: bfloat16 [8192, 4096], P('tm', 'batch'), parts along dimension 1, may hold values from -6 to 6
- rates: float32 [4096], P('batch'), parts along dimension 0, may hold values from 1.2207031e-05 to 0.5
- init_state: float32 [4096], P('batch'), parts along dimension 0, may hold values from -5 to 5
- recur_weight: bfloat16 [2048, 2048], replicated, may hold values from -0.5 to 0.5
Outputs:
- trajectory: float32 [8192, 4096], P('tm', 'batch'), parts along dimension 1
- step_norms: float32 [6], P('batch'), parts along dimension 0
The draws below stay inside these ranges and needn't reach their ends.
There are 2 independent parts, one for each index of `batch`. The reference program is written for one: setup_inputs(seed, part) draws one part's arguments, and reference() takes and returns one part's arrays. A program takes and returns all parts, laid end to end along the dimension named above; an argument that names none is the same for every part. Nothing has to cross between parts.
All inputs are finite; a program needn't handle non-finite values.
Results may differ from the reference program's by a relative error of at most 0.0012.
Values sent between devices are 32-bit elements; how exact they have to be, the bound alone decides.
A program may use at most 64 MiB of HBM per device.

```python
import jax
import jax.numpy as jnp
from jax import lax

H = 2048
ITERS = 3
TOKENS = 8192


def draw_gate_in(key, part):
    first_key, spot_key, height_key = jax.random.split(jax.random.fold_in(key, 11), 3)
    base = jnp.clip(jax.random.normal(first_key, (TOKENS, H)), -4.0, 4.0)
    spots = jax.random.randint(spot_key, (4,), 0, TOKENS)
    height = jax.random.uniform(height_key, (4,), minval=8.25, maxval=8.7)
    places = jnp.arange(TOKENS)
    level = jnp.max(jnp.where(places[:, None] == spots[None, :], height[None, :], -100.0), axis=1)
    return jnp.where(level[:, None] > 0.0, level[:, None] + 0.0 * base, base).astype(jnp.bfloat16)


def draw_rates(key, part):
    first_key = jax.random.fold_in(jax.random.fold_in(key, 23), 0)
    lowest = jnp.log(0.1 / TOKENS)
    values = jnp.exp(jax.random.uniform(first_key, (H,), minval=lowest, maxval=jnp.log(0.5)))
    return values.astype(jnp.float32)


def draw_recur_weight(key, part):
    body_key, size_key, sign_key = jax.random.split(jax.random.fold_in(key, 37), 3)
    spread = jnp.float32(H) ** (-0.5)
    inner = jnp.clip(jax.random.normal(body_key, (H, H)), -6.0, 6.0) * spread
    size = jnp.exp(jax.random.uniform(size_key, (H,), minval=jnp.log(0.2), maxval=jnp.log(0.5)))
    sign = jnp.where(jax.random.uniform(sign_key, (H,)) < 0.5, -1.0, 1.0)
    places = jnp.arange(H)
    on_diag = places[:, None] == places[None, :]
    values = jnp.where(on_diag, (size * sign)[:, None] + 0.0 * inner, inner)
    return values.astype(jnp.float32).astype(jnp.bfloat16)


def steps_of(own_key, extent, shards, low, largest):
    def one(position, blocks):
        steps = jax.random.uniform(jax.random.fold_in(jax.random.fold_in(own_key, 6), position), (blocks,), jnp.float32, low / len(shards), largest / len(shards))
        return jnp.repeat(jnp.exp(steps), extent[position] // blocks).reshape((-1,) + (1,) * (len(extent) - position - 1))

    gain = one(*shards[0])
    for cut in shards[1:]:
        gain = gain * one(*cut)
    return gain


def normal_values(rng, dims, scale, limit, shards=(), dtype=jnp.bfloat16):
    drawn = jax.random.normal(rng, dims, jnp.float32) * scale
    if len(shards) > 0:
        drawn = steps_of(rng, dims, shards, -0.22, 0.18) * drawn
    return jnp.clip(drawn, min=-limit, max=limit).astype(dtype)


def setup_inputs(seed: int = 0, part: int = 0) -> dict:
    seeds = jax.random.split(jax.random.key(seed), 6)
    part_keys = jax.random.split(jax.random.fold_in(seeds[5], part), 6)
    return {
        "gate_in": draw_gate_in(jax.random.fold_in(jax.random.fold_in(seeds[5], part), 71), part),
        "cand_in": normal_values(part_keys[1], (TOKENS, H), 1.0, 6.0, ((0, 128),)),
        "rates": draw_rates(jax.random.fold_in(jax.random.fold_in(seeds[5], part), 71), part),
        "init_state": normal_values(part_keys[3], (H,), 1.0, 5.0, (), jnp.float32),
        "recur_weight": draw_recur_weight(jax.random.fold_in(seeds[5], 71), part),
    }


def link(earlier, later):
    return (later[0] * earlier[0], later[0] * earlier[1] + later[1])

def reference(gate_in, cand_in, rates, init_state, recur_weight):
    gate = gate_in.astype(jnp.float32)
    keep = jnp.exp(-rates[None, :] * jax.nn.softplus(gate) - jnp.maximum(gate - 8.0, 0.0))
    cand_base = cand_in.astype(jnp.float32)
    unit_diag = jnp.diagonal(recur_weight).astype(jnp.float32)
    state = jnp.zeros(gate.shape, jnp.float32)
    totals = []
    for step in range(ITERS):
        prev = jnp.concatenate([init_state[None, :], state[:-1]], axis=0)
        mixed = jnp.dot(prev.astype(jnp.bfloat16), recur_weight, preferred_element_type=jnp.float32)
        cand = jnp.tanh(cand_base + mixed)
        mapped = keep * prev + (1.0 - keep) * cand
        slope = keep + (1.0 - keep) * (1.0 - cand * cand) * unit_diag[None, :]
        offset = mapped - slope * prev
        offset = jnp.concatenate([offset[:1] + slope[:1] * init_state[None, :], offset[1:]], axis=0)
        cum_a, fresh = lax.associative_scan(link, (slope, offset), axis=0)
        delta = fresh - state
        totals.append(jnp.sum(delta * delta))
        state = fresh
    return (state, jnp.sqrt(jnp.stack(totals) / (TOKENS * H)))
```

```python
import functools

import jax
import jax.numpy as jnp
from jax import lax
from jax.experimental import pallas as pl
from jax.experimental.pallas import tpu as pltpu
from jax.sharding import PartitionSpec as P

ITERS = 3
LANES = 128
ROWS = 64
BLOCKS = 8
STEPS = 8
MEMBERS = 8
MESH = pl.DeviceIdType.MESH


def joined(first, second):
    return second[0] * first[0], second[0] * first[1] + second[1]


def kernel(
    groups, tiles, scale,
    gate_hbm, cand_hbm, rates_hbm, init_hbm, weight_hbm,
    out_hbm, norms_ref,
    gate_v, cand_v, weight_v, rates_v, init_v,
    spread, keep_v, base_v, state_v, a_v, b_v, before_a, before_b, whole_a, whole_b,
    diag_v, entry_v, delta_v, low_v, first_low, mixed_v,
    sent1, got1, sent2, got2, start_v, sent3, got3, final_v,
    load_sem, weight_sem, send1, recv1, send2, recv2, send3, recv3, out_sem,
):
    f32 = jnp.float32
    place = lax.axis_index("tm")
    part = lax.axis_index("batch")
    group, member = place // MEMBERS, lax.rem(place, MEMBERS)
    devices = groups * MEMBERS
    width = tiles * LANES
    depth = width // 8

    def at(index):
        return (index, part)

    barrier = pltpu.get_barrier_semaphore()
    for d in range(1, MEMBERS):
        other = group * MEMBERS + lax.rem(member + d, MEMBERS)
        pl.semaphore_signal(barrier, inc=1, device_id=at(other), device_id_type=MESH)
    for d in range(1, groups):
        other = lax.rem(group + d, groups) * MEMBERS + member
        pl.semaphore_signal(barrier, inc=1, device_id=at(other), device_id_type=MESH)

    loads = [
        pltpu.make_async_copy(gate_hbm, gate_v, load_sem.at[0]),
        pltpu.make_async_copy(cand_hbm, cand_v, load_sem.at[1]),
        pltpu.make_async_copy(rates_hbm, rates_v, load_sem.at[2]),
        pltpu.make_async_copy(init_hbm, init_v, load_sem.at[3]),
    ]
    for copy in loads:
        copy.start()
    weight_copies = [
        pltpu.make_async_copy(
            weight_hbm.at[pl.ds(i * depth, depth)], weight_v.at[pl.ds(i * depth, depth)], weight_sem.at[i]
        )
        for i in range(8)
    ]
    for copy in weight_copies:
        copy.start()
    for copy in loads:
        copy.wait()

    block = lax.broadcasted_iota(jnp.int32, (BLOCKS, LANES), 0)
    entry_v[...] = jnp.where(place == 0, init_v[...], 0.0)

    for l in range(tiles):
        cols = pl.ds(l * LANES, LANES)
        spread[0, l] = gate_v[:, cols].astype(f32)
        spread[1, l] = cand_v[:, cols].astype(f32)
        rate = rates_v[pl.ds(l, 1), :]
        for j in range(STEPS):
            rows = pl.ds(j * BLOCKS, BLOCKS)
            gate = spread[0, l, pl.ds(j, BLOCKS, stride=STEPS), :]
            soft = jnp.maximum(gate, 0.0) + jnp.log1p(jnp.exp(-jnp.abs(gate)))
            keep_v[l, rows, :] = jnp.exp(-rate * soft - jnp.maximum(gate - 8.0, 0.0))
            base_v[l, rows, :] = spread[1, l, pl.ds(j, BLOCKS, stride=STEPS), :]

    top = lax.broadcasted_iota(jnp.int32, (16, LANES), 0) == 0
    for l in range(tiles):
        row = jnp.broadcast_to(entry_v[pl.ds(l, 1), :], (16, LANES))
        first_low[:, pl.ds(l * LANES, LANES)] = jnp.where(top, row, 0.0).astype(jnp.bfloat16)
    eye = lax.broadcasted_iota(jnp.int32, (LANES, LANES), 0) == lax.broadcasted_iota(
        jnp.int32, (LANES, LANES), 1
    )
    total = jnp.zeros((16, width), f32)
    for i, copy in enumerate(weight_copies):
        copy.wait()
        for l in range(i * tiles // 8, (i + 1) * tiles // 8):
            corner = weight_v[pl.ds(l * LANES, LANES), pl.ds(l * LANES, LANES)].astype(f32)
            diag_v[pl.ds(l, 1), :] = jnp.sum(jnp.where(eye, corner, 0.0), axis=0, keepdims=True)
        deep = pl.ds(i * depth, depth)
        total = total + jnp.dot(first_low[:, deep], weight_v[deep, :], preferred_element_type=f32)
    mixed_v[pl.ds(0, 16), :] = total

    def local_scan(k, l):
        cols = pl.ds(l * LANES, LANES)
        unit = diag_v[pl.ds(l, 1), :]
        a = b = old = None
        for j in range(STEPS):
            rows = pl.ds(j * BLOCKS, BLOCKS)
            keep = keep_v[l, rows, :]
            arg = base_v[l, rows, :]
            if k > 0 or j == 0:
                arg = arg + mixed_v[rows, cols]
            cand = jnp.tanh(arg)
            rest = 1.0 - keep
            slope = keep + rest * (1.0 - cand * cand) * unit
            step = rest * cand
            if j == 0:
                prev = jnp.broadcast_to(entry_v[pl.ds(l, 1), :], (BLOCKS, LANES))
                last = 0.0 if k == 0 else pltpu.roll(state_v[l, pl.ds(7 * BLOCKS, BLOCKS), :], 1, 0)
                prev = jnp.where(block == 0, prev, last)
                step = step + keep * prev
            elif k > 0:
                step = step + keep * old
            if k > 0:
                old = state_v[l, rows, :]
                step = step - old
            if j == 0:
                a, b = slope, step
            else:
                a, b = slope * a, slope * b + step
            a_v[l, rows, :] = a
            b_v[l, rows, :] = b
        for shift in (1, 2, 4):
            inside = block >= shift
            pa, pb = pltpu.roll(a, shift, 0), pltpu.roll(b, shift, 0)
            b = jnp.where(inside, a * pb + b, b)
            a = jnp.where(inside, a * pa, a)
        whole_a[pl.ds(l * BLOCKS, BLOCKS), :] = a
        whole_b[pl.ds(l * BLOCKS, BLOCKS), :] = b
        before_a[l] = jnp.where(block == 0, 1.0, pltpu.roll(a, 1, 0))
        before_b[l] = jnp.where(block == 0, 0.0, pltpu.roll(b, 1, 0))

    half = tiles // 2

    def exchange(k):
        for i in range(2):
            pick = pl.ds(i * half * BLOCKS + BLOCKS - 1, half, stride=BLOCKS)
            for first, source in ((0, whole_a), (tiles, whole_b)):
                value = source[pick, :]
                sent1[k, pl.ds(first + i * half, half), :] = value
                got1[k, member, pl.ds(first + i * half, half), :] = value
        if k == 0:
            pl.semaphore_wait(barrier, MEMBERS - 1 + groups - 1)
        for d in range(1, MEMBERS):
            other = group * MEMBERS + lax.rem(member + d, MEMBERS)
            pltpu.make_async_remote_copy(
                sent1.at[k], got1.at[k, member], send1.at[k], recv1.at[k],
                device_id=at(other), device_id_type=MESH,
            ).start()
        most = got1.at[k, pl.ds(0, MEMBERS - 1)]
        pltpu.make_async_copy(most, most, recv1.at[k]).wait()

        part_a, part_b = pl.ds(0, tiles), pl.ds(tiles, tiles)
        run = got1[k, 0, part_a, :], got1[k, 0, part_b, :]
        mine = jnp.ones((tiles, LANES), f32), jnp.zeros((tiles, LANES), f32)
        for m in range(1, MEMBERS):
            mine = tuple(jnp.where(member == m, new, old) for new, old in zip(run, mine))
            run = joined(run, (got1[k, m, part_a, :], got1[k, m, part_b, :]))
        sent2[k, part_a, :] = run[0]
        sent2[k, part_b, :] = run[1]
        for d in range(groups - 1, 0, -1):
            @pl.when(group + d < groups)
            def _():
                pltpu.make_async_remote_copy(
                    sent2.at[k], got2.at[k, group], send2.at[k, d], recv2.at[k, group],
                    device_id=at((group + d) * MEMBERS + member), device_id_type=MESH,
                ).start()
        start_v[...] = jnp.zeros((tiles, LANES), f32)
        for q in range(groups - 1):
            @pl.when(q < group)
            def _():
                slot = got2.at[k, q]
                pltpu.make_async_copy(slot, slot, recv2.at[k, q]).wait()
                start_v[...] = got2[k, q, part_a, :] * start_v[...] + got2[k, q, part_b, :]
        delta = mine[0] * start_v[...] + mine[1]
        delta_v[...] = delta
        entry_v[...] = entry_v[...] + delta

    def advance(k, l):
        cols = pl.ds(l * LANES, LANES)
        carry = before_b[l] + before_a[l] * delta_v[pl.ds(l, 1), :]
        change = jnp.zeros((BLOCKS, LANES), f32)
        states = []
        for j in range(STEPS):
            rows = pl.ds(j * BLOCKS, BLOCKS)
            moved = b_v[l, rows, :] + a_v[l, rows, :] * carry
            change = change + moved * moved
            new = moved if k == 0 else state_v[l, rows, :] + moved
            states.append(new)
            if k < ITERS - 1:
                state_v[l, rows, :] = new
            else:
                spread[0, l, pl.ds(j, BLOCKS, stride=STEPS), :] = new
        if k < ITERS - 1:
            head = jnp.broadcast_to(entry_v[pl.ds(l, 1), :], (BLOCKS, LANES))
            prevs = [jnp.where(block == 0, head, pltpu.roll(states[-1], 1, 0))] + states[:-1]
            for i in range(STEPS // 2):
                pair = jnp.concatenate(prevs[2 * i : 2 * i + 2], axis=0)
                low_v[pl.ds(i * 16, 16), cols] = pair.astype(jnp.bfloat16)
        else:
            pltpu.make_async_copy(spread.at[0, l], out_hbm.at[:, cols], out_sem.at[l]).start()
        return change

    lane = lax.broadcasted_iota(jnp.int32, (1, LANES), 1)
    totals = jnp.zeros((1, LANES), f32)
    for l in range(tiles):
        local_scan(0, l)
    for k in range(ITERS):
        exchange(k)
        change = jnp.zeros((BLOCKS, LANES), f32)
        for l in range(tiles):
            change = change + advance(k, l)
        totals = jnp.where(lane == k, jnp.sum(change), totals)
        if k < ITERS - 1:
            wide = 512
            for n in range(width // wide):
                cols = pl.ds(n * wide, wide)
                mixed_v[:, cols] = jnp.dot(low_v[...], weight_v[:, cols], preferred_element_type=f32)
                for l in range(n * wide // LANES, (n + 1) * wide // LANES):
                    local_scan(k + 1, l)

    sent3[...] = totals
    got3[place] = totals

    def send_total(d, carry):
        pltpu.make_async_remote_copy(
            sent3, got3.at[place], send3, recv3,
            device_id=at(lax.rem(place + d, devices)), device_id_type=MESH,
        ).start()
        return carry

    lax.fori_loop(1, devices, send_total, 0)
    most = got3.at[pl.ds(0, devices - 1)]
    for l in range(tiles):
        pltpu.make_async_copy(spread.at[0, l], out_hbm.at[:, pl.ds(l * LANES, LANES)], out_sem.at[l]).wait()
    for k in range(ITERS):
        sent = got1.at[k, pl.ds(0, MEMBERS - 1)]
        pltpu.make_async_copy(sent, sent, send1.at[k]).wait()
        for d in range(1, groups):
            @pl.when(group + d < groups)
            def _():
                pltpu.make_async_copy(sent2.at[k], sent2.at[k], send2.at[k, d]).wait()
    pltpu.make_async_copy(most, most, recv3).wait()
    pltpu.make_async_copy(most, most, send3).wait()
    norms_ref[...] = jnp.sqrt(jnp.sum(got3[...], axis=0) * scale)


def body(gate_in, cand_in, rates, init_state, recur_weight):
    rows, width = gate_in.shape
    devices = lax.axis_size("tm")
    groups, tiles = devices // MEMBERS, width // LANES
    f32, bf16 = jnp.float32, jnp.bfloat16
    hbm = pl.BlockSpec(memory_space=pltpu.HBM)
    dma = pltpu.SemaphoreType.DMA
    panel = pltpu.VMEM((tiles, rows, LANES), f32)
    edge = pltpu.VMEM((tiles, BLOCKS, LANES), f32)
    ends = pltpu.VMEM((tiles * BLOCKS, LANES), f32)
    units = pltpu.VMEM((tiles, LANES), f32)
    out, norms = pl.pallas_call(
        functools.partial(kernel, groups, tiles, 1.0 / (rows * devices * width)),
        out_shape=(
            jax.ShapeDtypeStruct((rows, width), f32),
            jax.ShapeDtypeStruct((1, LANES), f32),
        ),
        in_specs=[hbm] * 5,
        out_specs=(hbm, pl.BlockSpec(memory_space=pltpu.VMEM)),
        scratch_shapes=[
            pltpu.VMEM((rows, width), bf16),
            pltpu.VMEM((rows, width), bf16),
            pltpu.VMEM((width, width), bf16),
            units, units,
            pltpu.VMEM((2, tiles, rows, LANES), f32),
            panel, panel, panel, panel, panel, edge, edge, ends, ends,
            units, units, units,
            pltpu.VMEM((rows, width), bf16),
            pltpu.VMEM((16, width), bf16),
            pltpu.VMEM((rows, width), f32),
            pltpu.VMEM((ITERS, 2 * tiles, LANES), f32),
            pltpu.VMEM((ITERS, MEMBERS, 2 * tiles, LANES), f32),
            pltpu.VMEM((ITERS, 2 * tiles, LANES), f32),
            pltpu.VMEM((ITERS, groups, 2 * tiles, LANES), f32),
            units,
            pltpu.VMEM((1, LANES), f32),
            pltpu.VMEM((devices, 1, LANES), f32),
            pltpu.VMEM((8, LANES), f32),
            dma((4,)), dma((8,)),
            dma((ITERS,)), dma((ITERS,)),
            dma((ITERS, groups)), dma((ITERS, groups)),
            dma, dma, dma((tiles,)),
        ],
        compiler_params=pltpu.CompilerParams(collective_id=0, has_side_effects=True),
        name="newton",
    )(gate_in, cand_in, rates.reshape(tiles, LANES), init_state.reshape(tiles, LANES), recur_weight)
    return out, norms[0, :ITERS]


def solution(mesh):
    placed = (P("tm", "batch"), P("tm", "batch"), P("batch"), P("batch"), P())
    return jax.shard_map(
        body, mesh=mesh, in_specs=placed, out_specs=(P("tm", "batch"), P("batch")), check_vma=False
    )
```

```python
import functools

import jax
import jax.numpy as jnp
from jax import lax
from jax.experimental import pallas as pl
from jax.experimental.pallas import tpu as pltpu
from jax.sharding import PartitionSpec as P

ITERS = 3
LANES = 128
ROWS = 64
BLOCKS = 8
STEPS = 8
MEMBERS = 8
NY, NZ, NX = 4, 8, 4
MESH = pl.DeviceIdType.MESH


def joined(first, second):
    return second[0] * first[0], second[0] * first[1] + second[1]


def kernel(
    groups, tiles, scale,
    gate_hbm, cand_hbm, rates_hbm, init_hbm, weight_hbm,
    out_v, norms_ref,
    gate_v, cand_v, weight_v, rates_v, init_v,
    spread, keep_v, base_v, state_v, a_v, b_v, before_a, before_b, whole_a, whole_b,
    diag_v, entry_v, delta_v, low_v, first_low, mixed_v,
    sent1, got1, sent2, got2, start_v, sent3, got3, final_v,
    load_sem, weight_sem, send1, recv1, send2, recv2, send3, recv3,
):
    f32 = jnp.float32
    place = lax.axis_index("tm")
    part = lax.axis_index("batch")
    group, member = place // MEMBERS, lax.rem(place, MEMBERS)
    devices = groups * MEMBERS
    width = tiles * LANES
    depth = width // 8

    def at(index):
        return (index, part)

    x, z, y = lax.rem(place, NX), lax.rem(place // NX, NZ), place // (NX * NZ)
    low_z, high_z = lax.rem(z, 2), z // 2
    xs = [lax.rem(x + d, NX) for d in range(NX)]
    zs = [lax.rem(z + d, NZ) * NX for d in range(NZ)]
    ys = [lax.rem(y + d, NY) * (NZ * NX) for d in range(NY)]
    pair = (z - low_z) * NX + (1 - low_z) * NX
    beside = [ys[0] + pair + xs[d] for d in (2, 1, 3)]
    beside += [ys[0] + zs[0] + xs[2], ys[0] + pair + x, ys[0] + zs[0] + xs[1], ys[0] + zs[0] + xs[3]]
    across = [ys[dy] + lax.rem(z - low_z + dz, NZ) * NX + x for dy in range(NY) for dz in range(2, NZ)]
    across += [ys[dy] + at_z + x for dy in range(1, NY) for at_z in (zs[0], pair)]
    everyone = [
        ys[dy] + zs[dz] + xs[dx]
        for dz in (4, 3, 5, 2, 6, 1, 7, 0) for dy in (2, 1, 3, 0) for dx in (2, 1, 3, 0)
        if dy > 0 or dz > 0 or dx > 0
    ]
    side = jnp.where(low_z == 1, 1, NZ // 2 - 1)
    routes = []
    for dy in range(NY):
        for hops, dz, flip in ((3, NZ // 4, True), (2, side, False), (1, side, True), (0, 0, False)):
            if dy == 0 and hops == 0:
                continue
            to_z = lax.rem(high_z + dz, NZ // 2) * 2 + (1 - low_z if flip else low_z)
            other = ys[dy] + to_z * NX + x
            routes.append((min(dy, NY - dy) + hops, other))
    routes = [other for _, other in sorted(routes, key=lambda r: -r[0])]

    barrier = pltpu.get_barrier_semaphore()
    for other in beside + across:
        pl.semaphore_signal(barrier, inc=1, device_id=at(other), device_id_type=MESH)

    loads = [
        pltpu.make_async_copy(gate_hbm, gate_v, load_sem.at[0]),
        pltpu.make_async_copy(cand_hbm, cand_v, load_sem.at[1]),
        pltpu.make_async_copy(rates_hbm, rates_v, load_sem.at[2]),
        pltpu.make_async_copy(init_hbm, init_v, load_sem.at[3]),
    ]
    for copy in loads:
        copy.start()
    weight_copies = [
        pltpu.make_async_copy(
            weight_hbm.at[pl.ds(i * depth, depth)], weight_v.at[pl.ds(i * depth, depth)], weight_sem.at[i]
        )
        for i in range(8)
    ]
    for copy in weight_copies:
        copy.start()
    for copy in loads:
        copy.wait()

    block = lax.broadcasted_iota(jnp.int32, (BLOCKS, LANES), 0)
    entry_v[...] = jnp.where(place == 0, init_v[...], 0.0)

    for l in range(tiles):
        cols = pl.ds(l * LANES, LANES)
        spread[0, l] = gate_v[:, cols].astype(f32)
        spread[1, l] = cand_v[:, cols].astype(f32)
        rate = rates_v[pl.ds(l, 1), :]
        for j in range(STEPS):
            rows = pl.ds(j * BLOCKS, BLOCKS)
            gate = spread[0, l, pl.ds(j, BLOCKS, stride=STEPS), :]
            soft = jnp.maximum(gate, 0.0) + jnp.log1p(jnp.exp(-jnp.abs(gate)))
            keep_v[l, rows, :] = jnp.exp(-rate * soft - jnp.maximum(gate - 8.0, 0.0))
            base_v[l, rows, :] = spread[1, l, pl.ds(j, BLOCKS, stride=STEPS), :]

    top = lax.broadcasted_iota(jnp.int32, (16, LANES), 0) == 0
    for l in range(tiles):
        row = jnp.broadcast_to(entry_v[pl.ds(l, 1), :], (16, LANES))
        first_low[:, pl.ds(l * LANES, LANES)] = jnp.where(top, row, 0.0).astype(jnp.bfloat16)
    eye = lax.broadcasted_iota(jnp.int32, (LANES, LANES), 0) == lax.broadcasted_iota(
        jnp.int32, (LANES, LANES), 1
    )
    total = jnp.zeros((16, width), f32)
    for i, copy in enumerate(weight_copies):
        copy.wait()
        for l in range(i * tiles // 8, (i + 1) * tiles // 8):
            corner = weight_v[pl.ds(l * LANES, LANES), pl.ds(l * LANES, LANES)].astype(f32)
            diag_v[pl.ds(l, 1), :] = jnp.sum(jnp.where(eye, corner, 0.0), axis=0, keepdims=True)
        deep = pl.ds(i * depth, depth)
        total = total + jnp.dot(first_low[:, deep], weight_v[deep, :], preferred_element_type=f32)
    mixed_v[pl.ds(0, 16), :] = total

    def local_scan(k, l):
        cols = pl.ds(l * LANES, LANES)
        unit = diag_v[pl.ds(l, 1), :]
        a = b = old = None
        for j in range(STEPS):
            rows = pl.ds(j * BLOCKS, BLOCKS)
            keep = keep_v[l, rows, :]
            arg = base_v[l, rows, :]
            if k > 0 or j == 0:
                arg = arg + mixed_v[rows, cols]
            cand = jnp.tanh(arg)
            rest = 1.0 - keep
            slope = keep + rest * (1.0 - cand * cand) * unit
            step = rest * cand
            if j == 0:
                prev = jnp.broadcast_to(entry_v[pl.ds(l, 1), :], (BLOCKS, LANES))
                last = 0.0 if k == 0 else pltpu.roll(state_v[l, pl.ds(7 * BLOCKS, BLOCKS), :], 1, 0)
                prev = jnp.where(block == 0, prev, last)
                step = step + keep * prev
            elif k > 0:
                step = step + keep * old
            if k > 0:
                old = state_v[l, rows, :]
                step = step - old
            if j == 0:
                a, b = slope, step
            else:
                a, b = slope * a, slope * b + step
            a_v[l, rows, :] = a
            b_v[l, rows, :] = b
        for shift in (1, 2, 4):
            inside = block >= shift
            pa, pb = pltpu.roll(a, shift, 0), pltpu.roll(b, shift, 0)
            b = jnp.where(inside, a * pb + b, b)
            a = jnp.where(inside, a * pa, a)
        whole_a[pl.ds(l * BLOCKS, BLOCKS), :] = a
        whole_b[pl.ds(l * BLOCKS, BLOCKS), :] = b
        before_a[l] = jnp.where(block == 0, 1.0, pltpu.roll(a, 1, 0))
        before_b[l] = jnp.where(block == 0, 0.0, pltpu.roll(b, 1, 0))

    half = tiles // 2

    def exchange(k):
        for i in range(2):
            pick = pl.ds(i * half * BLOCKS + BLOCKS - 1, half, stride=BLOCKS)
            for first, source in ((0, whole_a), (tiles, whole_b)):
                value = source[pick, :]
                sent1[k, pl.ds(first + i * half, half), :] = value
                got1[k, member, pl.ds(first + i * half, half), :] = value
        if k == 0:
            pl.semaphore_wait(barrier, len(beside) + len(across))
        for other in beside:
            pltpu.make_async_remote_copy(
                sent1.at[k], got1.at[k, member], send1.at[k], recv1.at[k],
                device_id=at(other), device_id_type=MESH,
            ).start()
        most = got1.at[k, pl.ds(0, MEMBERS - 1)]
        pltpu.make_async_copy(most, most, recv1.at[k]).wait()

        part_a, part_b = pl.ds(0, tiles), pl.ds(tiles, tiles)
        run = got1[k, 0, part_a, :], got1[k, 0, part_b, :]
        mine = jnp.ones((tiles, LANES), f32), jnp.zeros((tiles, LANES), f32)
        for m in range(1, MEMBERS):
            mine = tuple(jnp.where(member == m, new, old) for new, old in zip(run, mine))
            run = joined(run, (got1[k, m, part_a, :], got1[k, m, part_b, :]))
        sent2[k, part_a, :] = run[0]
        sent2[k, part_b, :] = run[1]
        for i, other in enumerate(routes):
            @pl.when(other // MEMBERS > group)
            def _():
                pltpu.make_async_remote_copy(
                    sent2.at[k], got2.at[k, group], send2.at[k, i], recv2.at[k, group],
                    device_id=at(other), device_id_type=MESH,
                ).start()
        start_v[...] = jnp.zeros((tiles, LANES), f32)
        for q in range(groups - 1):
            @pl.when(q < group)
            def _():
                slot = got2.at[k, q]
                pltpu.make_async_copy(slot, slot, recv2.at[k, q]).wait()
                start_v[...] = got2[k, q, part_a, :] * start_v[...] + got2[k, q, part_b, :]
        delta = mine[0] * start_v[...] + mine[1]
        delta_v[...] = delta
        entry_v[...] = entry_v[...] + delta

    def advance(k, l):
        cols = pl.ds(l * LANES, LANES)
        carry = before_b[l] + before_a[l] * delta_v[pl.ds(l, 1), :]
        change = jnp.zeros((BLOCKS, LANES), f32)
        states = []
        for j in range(STEPS):
            rows = pl.ds(j * BLOCKS, BLOCKS)
            moved = b_v[l, rows, :] + a_v[l, rows, :] * carry
            change = change + moved * moved
            new = moved if k == 0 else state_v[l, rows, :] + moved
            states.append(new)
            if k < ITERS - 1:
                state_v[l, rows, :] = new
            else:
                out_v[l, pl.ds(j, BLOCKS, stride=STEPS), :] = new
        if k < ITERS - 1:
            head = jnp.broadcast_to(entry_v[pl.ds(l, 1), :], (BLOCKS, LANES))
            prevs = [jnp.where(block == 0, head, pltpu.roll(states[-1], 1, 0))] + states[:-1]
            for i in range(STEPS // 2):
                pair = jnp.concatenate(prevs[2 * i : 2 * i + 2], axis=0)
                low_v[pl.ds(i * 16, 16), cols] = pair.astype(jnp.bfloat16)
        return change

    lane = lax.broadcasted_iota(jnp.int32, (1, LANES), 1)
    totals = jnp.zeros((1, LANES), f32)
    for l in range(tiles):
        local_scan(0, l)
    for k in range(ITERS):
        exchange(k)
        change = jnp.zeros((BLOCKS, LANES), f32)
        for l in range(tiles):
            change = change + advance(k, l)
        totals = jnp.where(lane == k, jnp.sum(change), totals)
        if k < ITERS - 1:
            wide = 512
            for n in range(width // wide):
                cols = pl.ds(n * wide, wide)
                mixed_v[:, cols] = jnp.dot(low_v[...], weight_v[:, cols], preferred_element_type=f32)
                for l in range(n * wide // LANES, (n + 1) * wide // LANES):
                    local_scan(k + 1, l)

    sent3[...] = totals
    got3[place] = totals

    for other in everyone:
        pltpu.make_async_remote_copy(
            sent3, got3.at[place], send3, recv3, device_id=at(other), device_id_type=MESH
        ).start()
    most = got3.at[pl.ds(0, devices - 1)]
    for k in range(ITERS):
        sent = got1.at[k, pl.ds(0, MEMBERS - 1)]
        pltpu.make_async_copy(sent, sent, send1.at[k]).wait()
        for i, other in enumerate(routes):
            @pl.when(other // MEMBERS > group)
            def _():
                pltpu.make_async_copy(sent2.at[k], sent2.at[k], send2.at[k, i]).wait()
    pltpu.make_async_copy(most, most, recv3).wait()
    pltpu.make_async_copy(most, most, send3).wait()
    norms_ref[...] = jnp.sqrt(jnp.sum(got3[...], axis=0) * scale)


def write(panels, norms, out_hbm, norms_out, sem):
    copies = [
        pltpu.make_async_copy(panels.at[l], out_hbm.at[:, pl.ds(l * LANES, LANES)], sem.at[l])
        for l in range(panels.shape[0])
    ]
    for copy in copies:
        copy.start()
    norms_out[...] = norms[0, 0:ITERS]
    for copy in copies:
        copy.wait()


def body(gate_in, cand_in, rates, init_state, recur_weight):
    rows, width = gate_in.shape
    devices = lax.axis_size("tm")
    groups, tiles = devices // MEMBERS, width // LANES
    f32, bf16 = jnp.float32, jnp.bfloat16
    hbm = pl.BlockSpec(memory_space=pltpu.HBM)
    vmem = pl.BlockSpec(memory_space=pltpu.VMEM)
    dma = pltpu.SemaphoreType.DMA
    panel = pltpu.VMEM((tiles, rows, LANES), f32)
    edge = pltpu.VMEM((tiles, BLOCKS, LANES), f32)
    ends = pltpu.VMEM((tiles * BLOCKS, LANES), f32)
    units = pltpu.VMEM((tiles, LANES), f32)
    operands = (gate_in, cand_in, rates.reshape(tiles, LANES), init_state.reshape(tiles, LANES), recur_weight)
    operands = [pltpu.with_memory_space_constraint(v, pltpu.HBM) for v in operands]
    out, norms = pl.pallas_call(
        functools.partial(kernel, groups, tiles, 1.0 / (rows * devices * width)),
        out_shape=(
            jax.ShapeDtypeStruct((tiles, rows, LANES), f32),
            jax.ShapeDtypeStruct((1, LANES), f32),
        ),
        in_specs=[hbm] * 5,
        out_specs=(vmem, vmem),
        scratch_shapes=[
            pltpu.VMEM((rows, width), bf16),
            pltpu.VMEM((rows, width), bf16),
            pltpu.VMEM((width, width), bf16),
            units, units,
            pltpu.VMEM((2, tiles, rows, LANES), f32),
            panel, panel, panel, panel, panel, edge, edge, ends, ends,
            units, units, units,
            pltpu.VMEM((rows, width), bf16),
            pltpu.VMEM((16, width), bf16),
            pltpu.VMEM((rows, width), f32),
            pltpu.VMEM((ITERS, 2 * tiles, LANES), f32),
            pltpu.VMEM((ITERS, MEMBERS, 2 * tiles, LANES), f32),
            pltpu.VMEM((ITERS, 2 * tiles, LANES), f32),
            pltpu.VMEM((ITERS, groups, 2 * tiles, LANES), f32),
            units,
            pltpu.VMEM((1, LANES), f32),
            pltpu.VMEM((devices, 1, LANES), f32),
            pltpu.VMEM((8, LANES), f32),
            dma((4,)), dma((8,)),
            dma((ITERS,)), dma((ITERS,)),
            dma((ITERS, groups)), dma((ITERS, groups)),
            dma, dma,
        ],
        compiler_params=pltpu.CompilerParams(
            collective_id=0, has_side_effects=True, vmem_limit_bytes=32 * 1024 * 1024
        ),
        name="newton",
    )(*operands)
    return pl.pallas_call(
        write,
        out_shape=(
            jax.ShapeDtypeStruct((rows, width), f32),
            jax.ShapeDtypeStruct((ITERS,), f32),
        ),
        in_specs=[vmem, vmem],
        out_specs=(hbm, vmem),
        scratch_shapes=[dma((tiles,))],
        compiler_params=pltpu.CompilerParams(vmem_limit_bytes=4 * 1024 * 1024),
        name="write",
    )(out, norms)


def solution(mesh):
    placed = (P("tm", "batch"), P("tm", "batch"), P("batch"), P("batch"), P())
    return jax.shard_map(
        body, mesh=mesh, in_specs=placed, out_specs=(P("tm", "batch"), P("batch")), check_vma=False
    )
```

```python
import functools

import jax
import jax.numpy as jnp
from jax import lax
from jax.experimental import pallas as pl
from jax.experimental.pallas import tpu as pltpu
from jax.sharding import PartitionSpec as P

ITERS = 3
LANES = 128
ROWS = 64
BLOCKS = 8
STEPS = 8
MEMBERS = 8
NY, NZ, NX = 4, 8, 4
MESH = pl.DeviceIdType.MESH


def joined(first, second):
    return second[0] * first[0], second[0] * first[1] + second[1]


def kernel(
    groups, tiles, scale,
    gate_hbm, cand_hbm, rates_hbm, init_hbm, weight_hbm,
    out_v, norms_ref,
    gate_v, cand_v, weight_v, rates_v, init_v,
    spread, keep_v, base_v, state_v, a_v, b_v, before_a, before_b, whole_a, whole_b,
    diag_v, entry_v, delta_v, low_v, first_low, mixed_v,
    sent1, got1, sent2, got2, start_v, quad_v, got3, sent4, got4, sent5, got5,
    load_sem, weight_sem, send1, recv1, send2, recv2, send3, recv3, send4, recv4, send5, recv5,
):
    f32 = jnp.float32
    place = lax.axis_index("tm")
    part = lax.axis_index("batch")
    group, member = place // MEMBERS, lax.rem(place, MEMBERS)
    width = tiles * LANES
    depth = width // 8

    def at(index):
        return (index, part)

    x, z, y = lax.rem(place, NX), lax.rem(place // NX, NZ), place // (NX * NZ)
    low_z, high_z = lax.rem(z, 2), z // 2
    xs = [lax.rem(x + d, NX) for d in range(NX)]
    zs = [lax.rem(z + d, NZ) * NX for d in range(NZ)]
    ys = [lax.rem(y + d, NY) * (NZ * NX) for d in range(NY)]
    pair = (z - low_z) * NX + (1 - low_z) * NX
    beside = [ys[0] + pair + xs[d] for d in (2, 1, 3)]
    beside += [ys[0] + zs[0] + xs[2], ys[0] + pair + x, ys[0] + zs[0] + xs[1], ys[0] + zs[0] + xs[3]]
    across = [ys[dy] + lax.rem(z - low_z + dz, NZ) * NX + x for dy in range(NY) for dz in range(2, NZ)]
    across += [ys[dy] + at_z + x for dy in range(1, NY) for at_z in (zs[0], pair)]
    alike = [
        ys[dy] + zs[dz] + x
        for dz in (4, 2, 6, 0) for dy in (2, 1, 3, 0)
        if dy > 0 or dz > 0
    ]
    own = tiles // MEMBERS
    lane = lax.broadcasted_iota(jnp.int32, (1, LANES), 1)
    side = jnp.where(low_z == 1, 1, NZ // 2 - 1)
    routes = []
    for dy in range(NY):
        for hops, dz, flip in ((3, NZ // 4, True), (2, side, False), (1, side, True), (0, 0, False)):
            if dy == 0 and hops == 0:
                continue
            to_z = lax.rem(high_z + dz, NZ // 2) * 2 + (1 - low_z if flip else low_z)
            other = ys[dy] + to_z * NX + x
            routes.append((min(dy, NY - dy) + hops, other))
    routes = [other for _, other in sorted(routes, key=lambda r: -r[0])]

    barrier = pltpu.get_barrier_semaphore()
    for other in beside + across:
        pl.semaphore_signal(barrier, inc=1, device_id=at(other), device_id_type=MESH)

    loads = [
        pltpu.make_async_copy(gate_hbm, gate_v, load_sem.at[0]),
        pltpu.make_async_copy(cand_hbm, cand_v, load_sem.at[1]),
        pltpu.make_async_copy(rates_hbm, rates_v, load_sem.at[2]),
        pltpu.make_async_copy(init_hbm, init_v, load_sem.at[3]),
    ]
    for copy in loads:
        copy.start()
    weight_copies = [
        pltpu.make_async_copy(
            weight_hbm.at[pl.ds(i * depth, depth)], weight_v.at[pl.ds(i * depth, depth)], weight_sem.at[i]
        )
        for i in range(8)
    ]
    for copy in weight_copies:
        copy.start()
    for copy in loads:
        copy.wait()

    block = lax.broadcasted_iota(jnp.int32, (BLOCKS, LANES), 0)
    entry_v[...] = jnp.where(place == 0, init_v[...], 0.0)

    for l in range(tiles):
        cols = pl.ds(l * LANES, LANES)
        spread[0, l] = gate_v[:, cols].astype(f32)
        spread[1, l] = cand_v[:, cols].astype(f32)
        rate = rates_v[pl.ds(l, 1), :]
        for j in range(STEPS):
            rows = pl.ds(j * BLOCKS, BLOCKS)
            gate = spread[0, l, pl.ds(j, BLOCKS, stride=STEPS), :]
            soft = jnp.maximum(gate, 0.0) + jnp.log1p(jnp.exp(-jnp.abs(gate)))
            keep_v[l, rows, :] = jnp.exp(-rate * soft - jnp.maximum(gate - 8.0, 0.0))
            base_v[l, rows, :] = spread[1, l, pl.ds(j, BLOCKS, stride=STEPS), :]

    top = lax.broadcasted_iota(jnp.int32, (16, LANES), 0) == 0
    for l in range(tiles):
        row = jnp.broadcast_to(entry_v[pl.ds(l, 1), :], (16, LANES))
        first_low[:, pl.ds(l * LANES, LANES)] = jnp.where(top, row, 0.0).astype(jnp.bfloat16)
    eye = lax.broadcasted_iota(jnp.int32, (LANES, LANES), 0) == lax.broadcasted_iota(
        jnp.int32, (LANES, LANES), 1
    )
    total = jnp.zeros((16, width), f32)
    for i, copy in enumerate(weight_copies):
        copy.wait()
        for l in range(i * tiles // 8, (i + 1) * tiles // 8):
            corner = weight_v[pl.ds(l * LANES, LANES), pl.ds(l * LANES, LANES)].astype(f32)
            diag_v[pl.ds(l, 1), :] = jnp.sum(jnp.where(eye, corner, 0.0), axis=0, keepdims=True)
        deep = pl.ds(i * depth, depth)
        total = total + jnp.dot(first_low[:, deep], weight_v[deep, :], preferred_element_type=f32)
    mixed_v[pl.ds(0, 16), :] = total

    def local_scan(k, l):
        cols = pl.ds(l * LANES, LANES)
        unit = diag_v[pl.ds(l, 1), :]
        a = b = old = None
        for j in range(STEPS):
            rows = pl.ds(j * BLOCKS, BLOCKS)
            keep = keep_v[l, rows, :]
            arg = base_v[l, rows, :]
            if k > 0 or j == 0:
                arg = arg + mixed_v[rows, cols]
            cand = jnp.tanh(arg)
            rest = 1.0 - keep
            slope = keep + rest * (1.0 - cand * cand) * unit
            step = rest * cand
            if j == 0:
                prev = jnp.broadcast_to(entry_v[pl.ds(l, 1), :], (BLOCKS, LANES))
                last = 0.0 if k == 0 else pltpu.roll(state_v[l, pl.ds(7 * BLOCKS, BLOCKS), :], 1, 0)
                prev = jnp.where(block == 0, prev, last)
                step = step + keep * prev
            elif k > 0:
                step = step + keep * old
            if k > 0:
                old = state_v[l, rows, :]
                step = step - old
            if j == 0:
                a, b = slope, step
            else:
                a, b = slope * a, slope * b + step
            a_v[l, rows, :] = a
            b_v[l, rows, :] = b
        for shift in (1, 2, 4):
            inside = block >= shift
            pa, pb = pltpu.roll(a, shift, 0), pltpu.roll(b, shift, 0)
            b = jnp.where(inside, a * pb + b, b)
            a = jnp.where(inside, a * pa, a)
        whole_a[pl.ds(l * BLOCKS, BLOCKS), :] = a
        whole_b[pl.ds(l * BLOCKS, BLOCKS), :] = b
        before_a[l] = jnp.where(block == 0, 1.0, pltpu.roll(a, 1, 0))
        before_b[l] = jnp.where(block == 0, 0.0, pltpu.roll(b, 1, 0))

    half = tiles // 2

    def send_squares():
        constant = jnp.zeros((BLOCKS, LANES), f32)
        for l in range(tiles):
            owner, row = l // own, l % own
            line = jnp.zeros((BLOCKS, LANES), f32)
            square = jnp.zeros((BLOCKS, LANES), f32)
            for j in range(STEPS):
                rows = pl.ds(j * BLOCKS, BLOCKS)
                a = a_v[l, rows, :]
                u, v = b_v[l, rows, :] + a * before_b[l], a * before_a[l]
                constant, line, square = constant + u * u, line + u * v, square + v * v
            last = pl.ds(l * BLOCKS + BLOCKS - 1, 1)
            quad_v[owner, pl.ds(row, 1), :] = whole_a[last, :]
            quad_v[owner, pl.ds(own + row, 1), :] = whole_b[last, :]
            quad_v[owner, pl.ds(2 * own + row, 1), :] = jnp.sum(line, axis=0, keepdims=True)
            quad_v[owner, pl.ds(3 * own + row, 1), :] = jnp.sum(square, axis=0, keepdims=True)
        sent4[4 * own] = jnp.sum(constant, axis=0, keepdims=True)
        got3[member] = quad_v[member]
        for other in beside:
            pltpu.make_async_remote_copy(
                quad_v.at[lax.rem(other, MEMBERS)], got3.at[member], send3, recv3,
                device_id=at(other), device_id_type=MESH,
            ).start()

    def join_squares():
        most = got3.at[pl.ds(0, MEMBERS - 1)]
        pltpu.make_async_copy(most, most, recv3).wait()
        for row in range(own):
            pa, pb = jnp.ones((1, LANES), f32), jnp.zeros((1, LANES), f32)
            constant = line = square = jnp.zeros((1, LANES), f32)
            for m in range(MEMBERS):
                a, b, q, r = (got3[m, pl.ds(i * own + row, 1), :] for i in range(4))
                constant = constant + (2.0 * q + r * pb) * pb
                line = line + (q + r * pb) * pa
                square = square + r * pa * pa
                pa, pb = a * pa, a * pb + b
            for i, value in enumerate((pa, pb, line, square)):
                sent4[i * own + row] = value
            sent4[4 * own] = sent4[4 * own] + constant
        got4[group] = sent4[...]
        for other in alike:
            pltpu.make_async_remote_copy(
                sent4, got4.at[group], send4, recv4, device_id=at(other), device_id_type=MESH
            ).start()

    def sum_squares():
        most = got4.at[pl.ds(0, groups - 1)]
        pltpu.make_async_copy(most, most, recv4).wait()
        change = jnp.zeros((1, LANES), f32)
        found = jnp.zeros((1, LANES), f32)
        for row in range(own):
            delta = jnp.zeros((1, LANES), f32)
            for g in range(groups):
                a, b, q, r = (got4[g, i * own + row] for i in range(4))
                change = change + (2.0 * q + r * delta) * delta
                delta = a * delta + b
        for g in range(groups):
            change = change + got4[g, 4 * own]
            found = found + got4[g, 4 * own + 1]
        found = jnp.where(lane == ITERS - 1, jnp.sum(change), found)
        sent5[...] = found
        got5[member] = found
        for other in beside:
            pltpu.make_async_remote_copy(
                sent5, got5.at[member], send5, recv5, device_id=at(other), device_id_type=MESH
            ).start()

    def exchange(k):
        for i in range(2):
            pick = pl.ds(i * half * BLOCKS + BLOCKS - 1, half, stride=BLOCKS)
            for first, source in ((0, whole_a), (tiles, whole_b)):
                value = source[pick, :]
                sent1[k, pl.ds(first + i * half, half), :] = value
                got1[k, member, pl.ds(first + i * half, half), :] = value
        if k == 0:
            pl.semaphore_wait(barrier, len(beside) + len(across))
        for other in beside:
            pltpu.make_async_remote_copy(
                sent1.at[k], got1.at[k, member], send1.at[k], recv1.at[k],
                device_id=at(other), device_id_type=MESH,
            ).start()
        if k == ITERS - 1:
            send_squares()
        most = got1.at[k, pl.ds(0, MEMBERS - 1)]
        pltpu.make_async_copy(most, most, recv1.at[k]).wait()

        part_a, part_b = pl.ds(0, tiles), pl.ds(tiles, tiles)
        run = got1[k, 0, part_a, :], got1[k, 0, part_b, :]
        mine = jnp.ones((tiles, LANES), f32), jnp.zeros((tiles, LANES), f32)
        for m in range(1, MEMBERS):
            mine = tuple(jnp.where(member == m, new, old) for new, old in zip(run, mine))
            run = joined(run, (got1[k, m, part_a, :], got1[k, m, part_b, :]))
        sent2[k, part_a, :] = run[0]
        sent2[k, part_b, :] = run[1]
        for i, other in enumerate(routes):
            @pl.when(other // MEMBERS > group)
            def _():
                pltpu.make_async_remote_copy(
                    sent2.at[k], got2.at[k, group], send2.at[k, i], recv2.at[k, group],
                    device_id=at(other), device_id_type=MESH,
                ).start()
        if k == ITERS - 1:
            join_squares()
        start_v[...] = jnp.zeros((tiles, LANES), f32)
        for q in range(groups - 1):
            @pl.when(q < group)
            def _():
                slot = got2.at[k, q]
                pltpu.make_async_copy(slot, slot, recv2.at[k, q]).wait()
                start_v[...] = got2[k, q, part_a, :] * start_v[...] + got2[k, q, part_b, :]
        delta = mine[0] * start_v[...] + mine[1]
        delta_v[...] = delta
        entry_v[...] = entry_v[...] + delta

    def advance(k, l):
        cols = pl.ds(l * LANES, LANES)
        carry = before_b[l] + before_a[l] * delta_v[pl.ds(l, 1), :]
        change = jnp.zeros((BLOCKS, LANES), f32)
        states = []
        for j in range(STEPS):
            rows = pl.ds(j * BLOCKS, BLOCKS)
            moved = b_v[l, rows, :] + a_v[l, rows, :] * carry
            if k < ITERS - 1:
                change = change + moved * moved
            new = moved if k == 0 else state_v[l, rows, :] + moved
            states.append(new)
            if k < ITERS - 1:
                state_v[l, rows, :] = new
            else:
                out_v[l, pl.ds(j, BLOCKS, stride=STEPS), :] = new
        if k < ITERS - 1:
            head = jnp.broadcast_to(entry_v[pl.ds(l, 1), :], (BLOCKS, LANES))
            prevs = [jnp.where(block == 0, head, pltpu.roll(states[-1], 1, 0))] + states[:-1]
            for i in range(STEPS // 2):
                pair = jnp.concatenate(prevs[2 * i : 2 * i + 2], axis=0)
                low_v[pl.ds(i * 16, 16), cols] = pair.astype(jnp.bfloat16)
        return change

    totals = jnp.zeros((1, LANES), f32)
    for l in range(tiles):
        local_scan(0, l)
    for k in range(ITERS):
        exchange(k)
        change = jnp.zeros((BLOCKS, LANES), f32)
        for l in range(tiles):
            change = change + advance(k, l)
        if k < ITERS - 1:
            totals = jnp.where(lane == k, jnp.sum(change), totals)
            sent4[4 * own + 1] = totals
            wide = 512
            for n in range(width // wide):
                cols = pl.ds(n * wide, wide)
                mixed_v[:, cols] = jnp.dot(low_v[...], weight_v[:, cols], preferred_element_type=f32)
                for l in range(n * wide // LANES, (n + 1) * wide // LANES):
                    local_scan(k + 1, l)

    sum_squares()
    for k in range(ITERS):
        sent = got1.at[k, pl.ds(0, MEMBERS - 1)]
        pltpu.make_async_copy(sent, sent, send1.at[k]).wait()
        for i, other in enumerate(routes):
            @pl.when(other // MEMBERS > group)
            def _():
                pltpu.make_async_copy(sent2.at[k], sent2.at[k], send2.at[k, i]).wait()
    pltpu.make_async_copy(got3.at[pl.ds(0, MEMBERS - 1)], got3.at[pl.ds(0, MEMBERS - 1)], send3).wait()
    pltpu.make_async_copy(got4.at[pl.ds(0, groups - 1)], got4.at[pl.ds(0, groups - 1)], send4).wait()
    most = got5.at[pl.ds(0, MEMBERS - 1)]
    pltpu.make_async_copy(most, most, send5).wait()
    pltpu.make_async_copy(most, most, recv5).wait()
    norms_ref[...] = jnp.sqrt(jnp.sum(got5[...], axis=0) * scale)


def write(panels, norms, out_hbm, norms_out, sem):
    copies = [
        pltpu.make_async_copy(panels.at[l], out_hbm.at[:, pl.ds(l * LANES, LANES)], sem.at[l])
        for l in range(panels.shape[0])
    ]
    for copy in copies:
        copy.start()
    norms_out[...] = norms[0, 0:ITERS]
    for copy in copies:
        copy.wait()


def body(gate_in, cand_in, rates, init_state, recur_weight):
    rows, width = gate_in.shape
    devices = lax.axis_size("tm")
    groups, tiles = devices // MEMBERS, width // LANES
    f32, bf16 = jnp.float32, jnp.bfloat16
    hbm = pl.BlockSpec(memory_space=pltpu.HBM)
    vmem = pl.BlockSpec(memory_space=pltpu.VMEM)
    dma = pltpu.SemaphoreType.DMA
    panel = pltpu.VMEM((tiles, rows, LANES), f32)
    edge = pltpu.VMEM((tiles, BLOCKS, LANES), f32)
    ends = pltpu.VMEM((tiles * BLOCKS, LANES), f32)
    units = pltpu.VMEM((tiles, LANES), f32)
    operands = (gate_in, cand_in, rates.reshape(tiles, LANES), init_state.reshape(tiles, LANES), recur_weight)
    operands = [pltpu.with_memory_space_constraint(v, pltpu.HBM) for v in operands]
    out, norms = pl.pallas_call(
        functools.partial(kernel, groups, tiles, 1.0 / (rows * devices * width)),
        out_shape=(
            jax.ShapeDtypeStruct((tiles, rows, LANES), f32),
            jax.ShapeDtypeStruct((1, LANES), f32),
        ),
        in_specs=[hbm] * 5,
        out_specs=(vmem, vmem),
        scratch_shapes=[
            pltpu.VMEM((rows, width), bf16),
            pltpu.VMEM((rows, width), bf16),
            pltpu.VMEM((width, width), bf16),
            units, units,
            pltpu.VMEM((2, tiles, rows, LANES), f32),
            panel, panel, panel, panel, panel, edge, edge, ends, ends,
            units, units, units,
            pltpu.VMEM((rows, width), bf16),
            pltpu.VMEM((16, width), bf16),
            pltpu.VMEM((rows, width), f32),
            pltpu.VMEM((ITERS, 2 * tiles, LANES), f32),
            pltpu.VMEM((ITERS, MEMBERS, 2 * tiles, LANES), f32),
            pltpu.VMEM((ITERS, 2 * tiles, LANES), f32),
            pltpu.VMEM((ITERS, groups, 2 * tiles, LANES), f32),
            units,
            pltpu.VMEM((MEMBERS, 4 * tiles // MEMBERS, LANES), f32),
            pltpu.VMEM((MEMBERS, 4 * tiles // MEMBERS, LANES), f32),
            pltpu.VMEM((4 * tiles // MEMBERS + 2, 1, LANES), f32),
            pltpu.VMEM((groups, 4 * tiles // MEMBERS + 2, 1, LANES), f32),
            pltpu.VMEM((1, LANES), f32),
            pltpu.VMEM((MEMBERS, 1, LANES), f32),
            dma((4,)), dma((8,)),
            dma((ITERS,)), dma((ITERS,)),
            dma((ITERS, groups)), dma((ITERS, groups)),
            dma, dma, dma, dma, dma, dma,
        ],
        compiler_params=pltpu.CompilerParams(
            collective_id=0, has_side_effects=True, vmem_limit_bytes=32 * 1024 * 1024
        ),
        name="newton",
    )(*operands)
    return pl.pallas_call(
        write,
        out_shape=(
            jax.ShapeDtypeStruct((rows, width), f32),
            jax.ShapeDtypeStruct((ITERS,), f32),
        ),
        in_specs=[vmem, vmem],
        out_specs=(hbm, vmem),
        scratch_shapes=[dma((tiles,))],
        compiler_params=pltpu.CompilerParams(vmem_limit_bytes=4 * 1024 * 1024),
        name="write",
    )(out, norms)


def solution(mesh):
    placed = (P("tm", "batch"), P("tm", "batch"), P("batch"), P("batch"), P())
    return jax.shard_map(
        body, mesh=mesh, in_specs=placed, out_specs=(P("tm", "batch"), P("batch")), check_vma=False
    )
```
